32 devices in a mesh: scen: 2 (over y), col: 16 (over z, x, core).
Axes of the slice: x: 2, y: 2, z: 4, core: 2. Of those that a mesh axis runs over, the one named last changes fastest.
Arguments:
- border: float32 [4, 1536, 16384], P('scen', None, 'col'), may hold values from -6 to 6
- barrier: float32 [4, 1536], P('scen'), may hold values from 0.1 to 10
- row_counts: int32 [4], P('scen'), may hold values from 1024 to 1536, as said below
Outputs:
- factor_panel: float32 [16, 2, 512, 512], P('col', 'scen')
The draws below stay inside these ranges and needn't reach their ends.
Inputs may be any that keep to these rules, and one draw needn't show every extreme that they name: `row_counts`: every value lies between 1024 and 1536, and at least one scenario uses all 1536 rows.
All inputs are finite; a program needn't handle non-finite values.
Results may differ from the reference program's by a relative error of at most 0.0003.
Values sent between devices are 32-bit elements; how exact they have to be, the bound alone decides.
A program may use at most 64 MiB of HBM per device.

```python
import math
import jax
import jax.numpy as jnp
from jax import lax

NB = 16384
PANEL = 512
RMAX = 1536
SCEN = 4
N_SCEN = 2
N_COL = 16


def draw_row_counts(key, part):
    counts = jax.random.randint(jax.random.fold_in(key, 11), (SCEN,), 2 * RMAX // 3, RMAX + 1)
    chosen = jax.random.randint(jax.random.fold_in(key, 23), (), 0, SCEN)
    return jnp.where(jnp.arange(SCEN) == chosen, RMAX, counts).astype(jnp.int32)


def block_levels(key, dims, cuts, smallest, high):
    gain = 1.0
    for position, parts in cuts:
        steps = jax.random.uniform(jax.random.fold_in(jax.random.fold_in(key, 6), position), (parts,), jnp.float32, smallest / len(cuts), high / len(cuts))
        gain = gain * jnp.repeat(jnp.exp(steps), dims[position] // parts).reshape((-1,) + (1,) * (len(dims) - 1 - position))
    return gain


def gaussian(key, extent, scale, reach, pieces=(), held_as=jnp.bfloat16):
    result = jax.random.normal(key, extent, jnp.float32) * scale
    if len(pieces) > 0:
        result = block_levels(key, extent, pieces, -0.22, 0.18) * result
    return jnp.clip(result, min=-reach, max=reach).astype(held_as)


def setup_inputs(seed: int = 0) -> dict:
    key_of = jax.random.split(jax.random.key(seed), 4)
    return {
        "border": gaussian(key_of[0], (SCEN, RMAX, NB), 1.0, 6.0, ((0, 2), (2, 16)), jnp.float32),
        "barrier": jnp.clip(jnp.exp(math.log(10.0) - 4.6051702 * jax.random.uniform(key_of[1], (SCEN, RMAX), jnp.float32) ** block_levels(key_of[1], (SCEN, RMAX), ((0, 2),), -0.2, 0.2)), 0.1, 10.0),
        "row_counts": draw_row_counts(jax.random.fold_in(key_of[3], 71), 0),
    }


def reference(border, barrier, row_counts):
    positions = lax.iota(jnp.int32, RMAX)
    weights = jnp.where(positions[None, :] < row_counts[:, None], 1.0 / barrier, jnp.float32(0.0))
    split_cols = border.reshape(SCEN, RMAX, N_COL, NB // N_COL)
    panel_border = split_cols[:, :, :, :PANEL // N_COL].reshape(SCEN, RMAX, PANEL)

    def accumulate(carry, items):
        border_one, weight_one, panel_one = items
        weighted = border_one * weight_one[:, None]
        term = jnp.einsum('rc,rk->ck', weighted.astype(jnp.float32), panel_one.astype(jnp.float32), precision=lax.Precision.HIGHEST, preferred_element_type=jnp.float32)
        return (carry + term, None)
    schur, _ = lax.scan(accumulate, jnp.zeros((NB, PANEL), jnp.float32), (border, weights, panel_border))
    block = schur.reshape(N_COL, NB // N_COL, PANEL)[:, :PANEL // N_COL, :].reshape(PANEL, PANEL)
    lower = jnp.linalg.cholesky(block)
    solved = lax.linalg.triangular_solve(lower, schur, left_side=False, lower=True, transpose_a=True)
    return solved.reshape(N_COL, N_SCEN, NB // (N_COL * N_SCEN), PANEL)
```

```python
import jax
import jax.numpy as jnp
from jax import lax
from jax.experimental import pallas as pl
from jax.experimental.pallas import tpu as pltpu
from jax.sharding import PartitionSpec as P

PANEL = 512
TILE = 128
SUB = 8
TILES = PANEL // TILE
UPPER = [(j, k) for j in range(TILES) for k in range(j, TILES)]


def tree(xs):
    xs=list(xs)
    while len(xs)>1:
        xs=[xs[i]+xs[i+1] if i+1<len(xs) else xs[i] for i in range(0,len(xs),2)]
    return xs[0]

def inverse_factor(a):
    n=TILE//SUB
    lane = lax.broadcasted_iota(jnp.int32,(SUB,TILE),1)
    sub = lax.broadcasted_iota(jnp.int32,(SUB,TILE),0)
    rows=[a[SUB*t:SUB*(t+1)] for t in range(n)]
    out=[]
    B=lambda x: jnp.broadcast_to(x,(SUB,TILE))
    for g in range(n):
        c0=g*SUB
        d=rows[g]
        inb=(lane>=c0)&(lane<c0+SUB)
        cols=[B(d[:,c0+j:c0+j+1]) for j in range(SUB)]
        A={}
        for j in range(SUB):
            for i in range(j,SUB):
                A[i,j]=B(cols[j][i:i+1])
        r=[None]*SUB; dd=[None]*SUB; M={}
        for k in range(SUB):
            dd[k]=A[k,k]
            r[k]=1.0/dd[k]
            for i in range(k+1,SUB):
                M[i,k]=A[i,k]*r[k]
            for j in range(k+1,SUB):
                for i in range(j,SUB):
                    A[i,j]=A[i,j]-M[i,k]*A[j,k] if i!=j else A[i,j]-M[i,k]*A[i,k]
        N={}
        for j in range(SUB):
            for i in range(j+1,SUB):
                s=M[i,j]
                for k in range(j+1,i):
                    s=s+M[i,k]*N[k,j]
                N[i,j]=-s
        dp=jnp.where(inb, jnp.where(lane-c0==sub,1.0,0.0), d)
        drow=[B(dp[j:j+1]) for j in range(SUB)]
        ncol=[]
        for j in range(SUB-1):
            m=jnp.zeros((SUB,TILE),jnp.float32)
            for i in range(j+1,SUB):
                m=jnp.where(sub==i,N[i,j],m)
            ncol.append(m)
        u=tree([dp]+[ncol[j]*drow[j] for j in range(SUB-1)])
        dvec=dd[0]
        for i in range(1,SUB):
            dvec=jnp.where(sub==i,dd[i],dvec)
        out.append(jnp.where(lane<c0+SUB,u*lax.rsqrt(dvec),0.0))
        if g==n-1: break
        ub=[B(u[i:i+1])*r[i] for i in range(SUB)]
        Z=[tree([ub[j]]+[N[i,j]*ub[i] for i in range(j+1,SUB)]) for j in range(SUB)]
        for t in range(g+1,n):
            cb=[B(rows[t][:,c0+j:c0+j+1]) for j in range(SUB)]
            rows[t]=jnp.where(inb,0.0,rows[t])-tree([cb[j]*Z[j] for j in range(SUB)])
    return jnp.concatenate(out,axis=0)

def factor_kernel(a_ref, b_ref, inv_ref, t_ref):
    t_ref[...] = jnp.zeros_like(t_ref)
    for n, (j, k) in enumerate(UPPER):
        t_ref[j * TILE : (j + 1) * TILE, k * TILE : (k + 1) * TILE] = a_ref[n] + b_ref[n]
    eye = (
        lax.broadcasted_iota(jnp.int32, (TILE, TILE), 0)
        == lax.broadcasted_iota(jnp.int32, (TILE, TILE), 1)
    ).astype(jnp.float32)
    for j in range(TILES):
        t_ref[j * TILE : (j + 1) * TILE, PANEL + j * TILE : PANEL + (j + 1) * TILE] = eye

    @pl.loop(0, TILES)
    def _(j):
        here = pl.ds(pl.multiple_of(j * TILE, TILE), TILE)
        inv = inverse_factor(t_ref[here, here])
        scaled = jnp.dot(
            inv, t_ref[here, :], precision=lax.Precision.HIGHEST, preferred_element_type=jnp.float32
        )
        inv_ref[here, :] = scaled[:, PANEL:]
        lane = lax.broadcasted_iota(jnp.int32, (TILE, PANEL), 1)
        ahead = jnp.where(lane >= (j + 1) * TILE, scaled[:, :PANEL], 0.0).T
        for i in range(1, TILES):

            @pl.when(i > j)
            def _():
                part = slice(i * TILE, (i + 1) * TILE)
                t_ref[part, :] -= jnp.dot(
                    ahead[part],
                    scaled,
                    precision=lax.Precision.HIGHEST,
                    preferred_element_type=jnp.float32,
                )


def inverse_of_factor(mine, other):
    return pl.pallas_call(
        factor_kernel,
        out_shape=jax.ShapeDtypeStruct((PANEL, PANEL), jnp.float32),
        in_specs=[pl.BlockSpec(memory_space=pltpu.VMEM)] * 2,
        out_specs=pl.BlockSpec(memory_space=pltpu.VMEM),
        scratch_shapes=[pltpu.VMEM((PANEL, 2 * PANEL), jnp.float32)],
        cost_estimate=pl.CostEstimate(
            flops=2 * 10**10, bytes_accessed=3 * 10**6, transcendentals=PANEL
        ),
        name="factor",
    )(mine, other)


def body(border, barrier, row_counts):
    scen_here, capacity, own_cols = border.shape
    n_scen = lax.axis_size("scen")
    per_owner = PANEL // lax.axis_size("col")
    rows_owned = own_cols // n_scen
    depth = scen_here * capacity
    positions = lax.iota(jnp.int32, capacity)
    weights = jnp.where(positions[None, :] < row_counts[:, None], 1.0 / barrier, jnp.float32(0.0))
    panel_part = jnp.transpose(border[:, :, :per_owner], (2, 0, 1)).reshape(per_owner, depth)
    panel = lax.all_gather(panel_part, "col", axis=0, tiled=True)
    weighted = panel * weights.reshape(1, depth)
    block = jnp.einsum(
        "pr,qr->pq", weighted, panel, precision=lax.Precision.HIGH,
        preferred_element_type=jnp.float32,
    )
    upper = jnp.stack(
        [block[j * TILE : (j + 1) * TILE, k * TILE : (k + 1) * TILE] for j, k in UPPER]
    )
    if n_scen == 2:
        swap = [(0, 1), (1, 0)]
        upper_other = lax.ppermute(upper, "scen", swap)
    else:
        upper_other = lax.psum(upper, "scen") - upper
    part = jnp.einsum(
        "pr,rc->pc", weighted, border.reshape(depth, own_cols), precision=lax.Precision.HIGH,
        preferred_element_type=jnp.float32,
    )
    if n_scen == 2:
        me = lax.axis_index("scen")
        sent = lax.dynamic_slice_in_dim(part, (1 - me) * rows_owned, rows_owned, 1)
        kept = lax.dynamic_slice_in_dim(part, me * rows_owned, rows_owned, 1)
        owned = kept + lax.ppermute(sent, "scen", swap)
    else:
        owned = lax.psum_scatter(part, "scen", scatter_dimension=1, tiled=True)
    inverse = inverse_of_factor(upper, upper_other)
    solved = jnp.einsum(
        "qt,pq->tp", owned, inverse, precision=lax.Precision.HIGHEST,
        preferred_element_type=jnp.float32,
    )
    return solved.reshape(1, 1, rows_owned, PANEL)


def solution(mesh):
    placed = (P("scen", None, "col"), P("scen", None), P("scen"))
    return jax.shard_map(
        body, mesh=mesh, in_specs=placed, out_specs=P("col", "scen", None, None), check_vma=False
    )
```

```python
import jax
import jax.numpy as jnp
from jax import lax
from jax.experimental import pallas as pl
from jax.experimental.pallas import tpu as pltpu
from jax.sharding import PartitionSpec as P

PANEL = 512
TILE = 128
SUB = 8
TILES = PANEL // TILE
UPPER = [(j, k) for j in range(TILES) for k in range(j, TILES)]


def tree(xs):
    xs=list(xs)
    while len(xs)>1:
        xs=[xs[i]+xs[i+1] if i+1<len(xs) else xs[i] for i in range(0,len(xs),2)]
    return xs[0]

def inverse_factor(a):
    n=TILE//SUB
    lane = lax.broadcasted_iota(jnp.int32,(SUB,TILE),1)
    sub = lax.broadcasted_iota(jnp.int32,(SUB,TILE),0)
    rows=[a[SUB*t:SUB*(t+1)] for t in range(n)]
    out=[]
    B=lambda x: jnp.broadcast_to(x,(SUB,TILE))
    for g in range(n):
        c0=g*SUB
        d=rows[g]
        inb=(lane>=c0)&(lane<c0+SUB)
        cols=[B(d[:,c0+j:c0+j+1]) for j in range(SUB)]
        A={}
        for j in range(SUB):
            for i in range(j,SUB):
                A[i,j]=B(cols[j][i:i+1])
        r=[None]*SUB; dd=[None]*SUB; M={}
        for k in range(SUB):
            dd[k]=A[k,k]
            r[k]=1.0/dd[k]
            for i in range(k+1,SUB):
                M[i,k]=A[i,k]*r[k]
            for j in range(k+1,SUB):
                for i in range(j,SUB):
                    A[i,j]=A[i,j]-M[i,k]*A[j,k] if i!=j else A[i,j]-M[i,k]*A[i,k]
        N={}
        for j in range(SUB):
            for i in range(j+1,SUB):
                s=M[i,j]
                for k in range(j+1,i):
                    s=s+M[i,k]*N[k,j]
                N[i,j]=-s
        dp=jnp.where(inb, jnp.where(lane-c0==sub,1.0,0.0), d)
        drow=[B(dp[j:j+1]) for j in range(SUB)]
        ncol=[]
        for j in range(SUB-1):
            m=jnp.zeros((SUB,TILE),jnp.float32)
            for i in range(j+1,SUB):
                m=jnp.where(sub==i,N[i,j],m)
            ncol.append(m)
        u=tree([dp]+[ncol[j]*drow[j] for j in range(SUB-1)])
        dvec=dd[0]
        for i in range(1,SUB):
            dvec=jnp.where(sub==i,dd[i],dvec)
        out.append(jnp.where(lane<c0+SUB,u*lax.rsqrt(dvec),0.0))
        if g==n-1: break
        ub=[B(u[i:i+1])*r[i] for i in range(SUB)]
        Z=[tree([ub[j]]+[N[i,j]*ub[i] for i in range(j+1,SUB)]) for j in range(SUB)]
        for t in range(g+1,n):
            cb=[B(rows[t][:,c0+j:c0+j+1]) for j in range(SUB)]
            rows[t]=jnp.where(inb,0.0,rows[t])-tree([cb[j]*Z[j] for j in range(SUB)])
    return jnp.concatenate(out,axis=0)

def factor_kernel(a_ref, b_ref, inv_ref, t_ref):
    t_ref[...] = jnp.zeros_like(t_ref)
    for n, (j, k) in enumerate(UPPER):
        t_ref[j * TILE : (j + 1) * TILE, k * TILE : (k + 1) * TILE] = a_ref[n] + b_ref[n]
    eye = (
        lax.broadcasted_iota(jnp.int32, (TILE, TILE), 0)
        == lax.broadcasted_iota(jnp.int32, (TILE, TILE), 1)
    ).astype(jnp.float32)
    for j in range(TILES):
        t_ref[j * TILE : (j + 1) * TILE, PANEL + j * TILE : PANEL + (j + 1) * TILE] = eye

    @pl.loop(0, TILES)
    def _(j):
        here = pl.ds(pl.multiple_of(j * TILE, TILE), TILE)
        inv = inverse_factor(t_ref[here, here])
        scaled = jnp.dot(
            inv, t_ref[here, :], precision=lax.Precision.HIGHEST, preferred_element_type=jnp.float32
        )
        inv_ref[here, :] = scaled[:, PANEL:]
        lane = lax.broadcasted_iota(jnp.int32, (TILE, PANEL), 1)
        ahead = jnp.where(lane >= (j + 1) * TILE, scaled[:, :PANEL], 0.0).T
        for i in range(1, TILES):

            @pl.when(i > j)
            def _():
                part = slice(i * TILE, (i + 1) * TILE)
                t_ref[part, :] -= jnp.dot(
                    ahead[part],
                    scaled,
                    precision=lax.Precision.HIGHEST,
                    preferred_element_type=jnp.float32,
                )


def inverse_of_factor(mine, other):
    return pl.pallas_call(
        factor_kernel,
        out_shape=jax.ShapeDtypeStruct((PANEL, PANEL), jnp.float32),
        in_specs=[pl.BlockSpec(memory_space=pltpu.VMEM)] * 2,
        out_specs=pl.BlockSpec(memory_space=pltpu.VMEM),
        scratch_shapes=[pltpu.VMEM((PANEL, 2 * PANEL), jnp.float32)],
        cost_estimate=pl.CostEstimate(
            flops=2 * 10**10, bytes_accessed=3 * 10**6, transcendentals=PANEL
        ),
        name="factor",
    )(mine, other)


def general_body(border, barrier, row_counts):
    scen_here, capacity, own_cols = border.shape
    n_scen = lax.axis_size("scen")
    per_owner = PANEL // lax.axis_size("col")
    rows_owned = own_cols // n_scen
    depth = scen_here * capacity
    positions = lax.iota(jnp.int32, capacity)
    weights = jnp.where(positions[None, :] < row_counts[:, None], 1.0 / barrier, jnp.float32(0.0))
    panel_part = jnp.transpose(border[:, :, :per_owner], (2, 0, 1)).reshape(per_owner, depth)
    panel = lax.all_gather(panel_part, "col", axis=0, tiled=True)
    weighted = panel * weights.reshape(1, depth)
    block = jnp.einsum(
        "pr,qr->pq", weighted, panel, precision=lax.Precision.HIGH,
        preferred_element_type=jnp.float32,
    )
    upper = jnp.stack(
        [block[j * TILE : (j + 1) * TILE, k * TILE : (k + 1) * TILE] for j, k in UPPER]
    )
    if n_scen == 2:
        swap = [(0, 1), (1, 0)]
        upper_other = lax.ppermute(upper, "scen", swap)
    else:
        upper_other = lax.psum(upper, "scen") - upper
    part = jnp.einsum(
        "pr,rc->pc", weighted, border.reshape(depth, own_cols), precision=lax.Precision.HIGH,
        preferred_element_type=jnp.float32,
    )
    if n_scen == 2:
        me = lax.axis_index("scen")
        sent = lax.dynamic_slice_in_dim(part, (1 - me) * rows_owned, rows_owned, 1)
        kept = lax.dynamic_slice_in_dim(part, me * rows_owned, rows_owned, 1)
        owned = kept + lax.ppermute(sent, "scen", swap)
    else:
        owned = lax.psum_scatter(part, "scen", scatter_dimension=1, tiled=True)
    inverse = inverse_of_factor(upper, upper_other)
    solved = jnp.einsum(
        "qt,pq->tp", owned, inverse, precision=lax.Precision.HIGHEST,
        preferred_element_type=jnp.float32,
    )
    return solved.reshape(1, 1, rows_owned, PANEL)


MESH = pl.DeviceIdType.MESH
CHUNK = 256
LAG = 3


def split(x):
    hi = x.astype(jnp.bfloat16)
    return hi, (x - hi.astype(jnp.float32)).astype(jnp.bfloat16)


def exact(a, b):
    return jnp.dot(a, b, precision=lax.Precision.HIGHEST, preferred_element_type=jnp.float32)


def bf16_nt(a, b):
    return lax.dot_general(a, b, (((1,), (1,)), ((), ())), preferred_element_type=jnp.float32)


def bf16_nn(a, b):
    return jnp.dot(a, b, preferred_element_type=jnp.float32)


def ring_kernel(
    part_ref, w_ref, border_ref, out_ref,
    gath, stage, bhi, blo, phi, plo, whi, wlo,
    u_keep, u_send, u_recv, g_own, g_recv, t_ref, inv_ref, low_ref, x_ref,
    stage_sem, ring_send, core_send, recv_sem, uy_send, uy_recv, gy_send, gy_recv,
):
    chips = lax.axis_size("col") // 2
    half_ring = chips // 2
    me = lax.axis_index("col")
    scen = lax.axis_index("scen")
    core = me % 2
    chip = me // 2
    pos = (1 - chip % 2) * (chip // 2) + (chip % 2) * (chips - 1 - chip // 2)
    depth_half = part_ref.shape[2]
    per = part_ref.shape[1]
    depth = 2 * depth_half
    cols = border_ref.shape[1]
    rows_owned = cols // 2

    def chip_at(p):
        p = (p + 2 * chips) % chips
        x = p // half_ring
        z = (1 - x) * p + x * (chips - 1 - p)
        return 2 * z + x

    up = {"col": 2 * chip_at(pos + 1) + core}
    down = {"col": 2 * chip_at(pos - 1) + core}
    mate = {"col": 2 * chip + 1 - core}
    across = {"scen": 1 - scen}

    barrier = pltpu.get_barrier_semaphore()
    for peer in (up, down, mate, across):
        pl.semaphore_signal(barrier, inc=1, device_id=peer, device_id_type=MESH)

    def fetch(n):
        return pltpu.make_async_copy(
            border_ref.at[pl.ds(pl.multiple_of(n * CHUNK, CHUNK), CHUNK)],
            stage.at[n % LAG],
            stage_sem.at[n % LAG],
        )

    chunks = depth // CHUNK
    for n in range(LAG):
        fetch(n).start()
    pl.semaphore_wait(barrier, 4)

    def send(src, block, h, send_sem, peer):
        return pltpu.make_async_remote_copy(
            src_ref=src,
            dst_ref=gath.at[block, h],
            send_sem=send_sem,
            recv_sem=recv_sem.at[block, h],
            device_id=peer,
            device_id_type=MESH,
        )

    def own(h, d):
        sem = core_send.at[0, h] if d == 2 else ring_send.at[d, 0, h]
        return send(part_ref.at[h], me, h, sem, (up, down, mate)[d])

    def block_of(d, k):
        return 2 * chip_at(pos - k if d == 0 else pos + k) + core

    def forward(d, k, h):
        block = block_of(d, k)
        return send(gath.at[block, h], block, h, ring_send.at[d, k, h], (up, down)[d])

    def push(d, k, h):
        block = block_of(d, k)
        return send(gath.at[block, h], block, h, core_send.at[2 * k - d, h], mate)

    def arrived(block, h):
        pltpu.make_async_copy(part_ref.at[h], gath.at[block, h], recv_sem.at[block, h]).wait()

    for h in range(2):
        for d in range(3):
            own(h, d).start()

    def convert_border(first):
        @pl.loop(first, first + chunks // 2)
        def _(n):
            fetch(n).wait()
            here = pl.ds(pl.multiple_of(n * CHUNK, CHUNK), CHUNK)
            hi, lo = split(stage[n % LAG])
            bhi[here, :] = hi
            blo[here, :] = lo

            @pl.when(n + LAG < chunks)
            def _():
                fetch(n + LAG).start()

    def convert(which, cc, src):
        for h in range(2):
            there = (which, pl.ds(cc * per, per), pl.ds(h * depth_half, depth_half))
            x = src(h)
            phi[there], plo[there] = split(x)
            whi[there], wlo[there] = split(x * w_ref[h])

    def convert_both(which):
        for cc in range(2):
            convert(which, cc, lambda h: gath[2 * which + cc, h])

    def unit(k):
        first = chip_at(pos - k)
        return first, chip_at(pos + k * (1 - k // half_ring))

    def product(k, which, dst):
        a, b = unit(k)
        left = jnp.concatenate([whi[a], whi[b], wlo[a], wlo[b]], axis=0)
        rows = 2 * whi.shape[1]

        @pl.loop(0, rows_owned // CHUNK)
        def _(n):
            col = pl.ds(pl.multiple_of(which * rows_owned + n * CHUNK, CHUNK), CHUNK)
            to = pl.ds(pl.multiple_of(n * CHUNK, CHUNK), CHUNK)
            both = bf16_nn(left, bhi[:, col])
            res = both[:rows] + both[rows:] + bf16_nn(left[:rows], blo[:, col])
            dst[a, :, to] = res[: rows // 2]
            dst[b, :, to] = res[rows // 2 :]

    def cross(which):
        return pltpu.make_async_remote_copy(
            src_ref=u_send.at[which],
            dst_ref=u_recv.at[which],
            send_sem=uy_send.at[which],
            recv_sem=uy_recv.at[which],
            device_id=across,
            device_id_type=MESH,
        )

    def product_send(k):
        product(k, 1 - scen, u_send)
        for which in unit(k):
            cross(which).start()

    def g_piece(n):
        row = max(n - 1, 0)
        first, last = (0, TILE) if n == 0 else (max(row, 1) * TILE, PANEL)
        at = (row, slice(None), slice(first, last))
        return pltpu.make_async_remote_copy(
            src_ref=g_own.at[at],
            dst_ref=g_recv.at[at],
            send_sem=gy_send.at[n],
            recv_sem=gy_recv.at[n],
            device_id=across,
            device_id_type=MESH,
        )

    def gram(i):
        pair = 2 * i
        rows = TILE
        left = jnp.concatenate([whi[pair], whi[pair + 1], wlo[pair], wlo[pair + 1]], axis=0)
        count = 2 * (TILES - i)
        right_hi = phi[pair : pair + count].reshape(count * 2 * per, depth)
        right_lo = plo[pair : pair + count].reshape(count * 2 * per, depth)
        both = bf16_nt(left, right_hi)
        g_own[i, :, i * TILE :] = both[:rows] + both[rows:] + bf16_nt(left[:rows], right_lo)

    @pl.loop(1, half_ring + 2)
    def _(k):
        @pl.when(k == 1)
        def _():
            convert_border(0)

        @pl.when(k <= half_ring)
        def _():
            arrived(block_of(0, k), 0)
            push(0, k, 0).start()

        @pl.when(k < half_ring)
        def _():
            forward(0, k, 0).start()
            arrived(block_of(1, k), 0)
            push(1, k, 0).start()

            @pl.when(k < half_ring - 1)
            def _():
                forward(1, k, 0).start()

        @pl.when(k == 1)
        def _():
            convert_border(chunks // 2)

        @pl.when(k == half_ring + 1)
        def _():
            for i in range(TILES):
                gram(i)
                if i == 0:
                    g_piece(0).start()
                g_piece(i + 1).start()

        @pl.when(k > 1)
        def _():
            product_send(k - 1)

        @pl.when(k <= half_ring)
        def _():
            arrived(block_of(1, k), 1)
            push(1, k, 1).start()

        @pl.when(k < half_ring)
        def _():
            forward(1, k, 1).start()
            arrived(block_of(0, k), 1)
            push(0, k, 1).start()

            @pl.when(k < half_ring - 1)
            def _():
                forward(0, k, 1).start()

        @pl.when(k > 1)
        def _():
            product(k - 1, scen, u_keep)

        @pl.when(k <= half_ring)
        def _():
            for d in range(2):
                @pl.when(k + d <= half_ring)
                def _():
                    which = block_of(d, k) // 2
                    for h in range(2):
                        arrived(2 * which + 1 - core, h)
                    convert_both(which)

        @pl.when(k == 1)
        def _():
            for h in range(2):
                arrived(2 * chip + 1 - core, h)
            convert(chip, core, lambda h: part_ref[h])
            convert(chip, 1 - core, lambda h: gath[2 * chip + 1 - core, h])


    t_ref[...] = jnp.zeros_like(t_ref)
    g_piece(0).wait_recv()
    t_ref[:TILE, :TILE] = g_own[0, :, :TILE] + g_recv[0, :, :TILE]

    @pl.loop(0, TILES)
    def _(j):
        here = pl.ds(pl.multiple_of(j * TILE, TILE), TILE)
        inv = inverse_factor(t_ref[here, here])
        inv_ref[j] = inv

        @pl.when(j == 0)
        def _():
            for i in range(TILES):
                g_piece(i + 1).wait_recv()
                lanes = slice(max(i, 1) * TILE, PANEL)
                t_ref[i * TILE : (i + 1) * TILE, lanes] = g_own[i, :, lanes] + g_recv[i, :, lanes]

        scaled = exact(inv, t_ref[here, :])
        lane = lax.broadcasted_iota(jnp.int32, (TILE, PANEL), 1)
        ahead = jnp.where(lane >= (j + 1) * TILE, scaled, 0.0).T
        low_ref[:, here] = ahead
        for i in range(1, TILES):

            @pl.when(i > j)
            def _():
                part = slice(i * TILE, (i + 1) * TILE)
                t_ref[part, :] -= exact(ahead[part], scaled)

    for which in range(chips):
        cross(which).wait_recv()
    for j in range(TILES):
        pair = slice(2 * j, 2 * j + 2)
        v = (u_keep[pair] + u_recv[pair]).reshape(TILE, rows_owned)
        if j > 0:
            v -= exact(low_ref[j * TILE : (j + 1) * TILE, : j * TILE], x_ref[: j * TILE, :])
        x = exact(inv_ref[j], v)
        x_ref[j * TILE : (j + 1) * TILE, :] = x
        out_ref[:, j * TILE : (j + 1) * TILE] = x.T

    for h in range(2):
        for d in range(3):
            own(h, d).wait_send()
    for k in range(1, half_ring + 1):
        for d in range(2):
            for h in range(2):
                if k < half_ring - 1 or (k < half_ring and d == h):
                    forward(d, k, h).wait_send()
                if k < half_ring or d == h:
                    push(d, k, h).wait_send()
    for which in range(chips):
        cross(which).wait_send()
    for n in range(TILES + 1):
        g_piece(n).wait_send()


def ring_body(border, barrier, row_counts):
    scen_here, capacity, own_cols = border.shape
    n_col = lax.axis_size("col")
    chips = n_col // 2
    per = PANEL // n_col
    depth = scen_here * capacity
    rows_owned = own_cols // lax.axis_size("scen")
    positions = lax.iota(jnp.int32, capacity)
    weights = jnp.where(positions[None, :] < row_counts[:, None], 1.0 / barrier, jnp.float32(0.0))
    part = jnp.transpose(border[:, :, :per], (0, 2, 1))
    dma = pltpu.SemaphoreType.DMA
    f32, bf16 = jnp.float32, jnp.bfloat16
    solved = pl.pallas_call(
        ring_kernel,
        out_shape=jax.ShapeDtypeStruct((rows_owned, PANEL), f32),
        in_specs=[
            pl.BlockSpec(memory_space=pltpu.VMEM),
            pl.BlockSpec(memory_space=pltpu.VMEM),
            pl.BlockSpec(memory_space=pl.ANY),
        ],
        out_specs=pl.BlockSpec(memory_space=pltpu.VMEM),
        scratch_shapes=[
            pltpu.VMEM((n_col, scen_here, per, capacity), f32),
            pltpu.VMEM((LAG, CHUNK, own_cols), f32),
            pltpu.VMEM((depth, own_cols), bf16),
            pltpu.VMEM((depth, own_cols), bf16),
            *[pltpu.VMEM((chips, 2 * per, depth), bf16)] * 4,
            *[pltpu.VMEM((chips, 2 * per, rows_owned), f32)] * 3,
            *[pltpu.VMEM((TILES, TILE, PANEL), f32)] * 2,
            pltpu.VMEM((PANEL, PANEL), f32),
            pltpu.VMEM((TILES, TILE, TILE), f32),
            pltpu.VMEM((PANEL, PANEL), f32),
            pltpu.VMEM((PANEL, rows_owned), f32),
            dma((LAG,)),
            dma((2, chips // 2, 2)),
            dma((chips + 1, 2)),
            dma((n_col, 2)),
            dma((chips,)),
            dma((chips,)),
            dma((TILES + 1,)),
            dma((TILES + 1,)),
        ],
        compiler_params=pltpu.CompilerParams(
            collective_id=0, has_side_effects=True, vmem_limit_bytes=60 * 2**20
        ),
        name="ring",
    )(part, weights.reshape(scen_here, 1, capacity), border.reshape(depth, own_cols))
    return solved.reshape(1, 1, rows_owned, PANEL)


def solution(mesh):
    n_scen, n_col = mesh.shape["scen"], mesh.shape["col"]
    ring = n_scen == 2 and 4 * (PANEL // n_col) == TILE
    placed = (P("scen", None, "col"), P("scen", None), P("scen"))
    return jax.shard_map(
        ring_body if ring else general_body,
        mesh=mesh,
        in_specs=placed,
        out_specs=P("col", "scen", None, None),
        check_vma=False,
    )
```

```python
import jax
import jax.numpy as jnp
from jax import lax
from jax.experimental import pallas as pl
from jax.experimental.pallas import tpu as pltpu
from jax.sharding import PartitionSpec as P

PANEL = 512
TILE = 128
SUB = 8
TILES = PANEL // TILE
UPPER = [(j, k) for j in range(TILES) for k in range(j, TILES)]


def tree(xs):
    xs=list(xs)
    while len(xs)>1:
        xs=[xs[i]+xs[i+1] if i+1<len(xs) else xs[i] for i in range(0,len(xs),2)]
    return xs[0]

def inverse_factor(a):
    n=TILE//SUB
    lane = lax.broadcasted_iota(jnp.int32,(SUB,TILE),1)
    sub = lax.broadcasted_iota(jnp.int32,(SUB,TILE),0)
    rows=[a[SUB*t:SUB*(t+1)] for t in range(n)]
    out=[]
    B=lambda x: jnp.broadcast_to(x,(SUB,TILE))
    for g in range(n):
        c0=g*SUB
        d=rows[g]
        inb=(lane>=c0)&(lane<c0+SUB)
        cols=[B(d[:,c0+j:c0+j+1]) for j in range(SUB)]
        A={}
        for j in range(SUB):
            for i in range(j,SUB):
                A[i,j]=B(cols[j][i:i+1])
        r=[None]*SUB; dd=[None]*SUB; M={}
        for k in range(SUB):
            dd[k]=A[k,k]
            r[k]=1.0/dd[k]
            for i in range(k+1,SUB):
                M[i,k]=A[i,k]*r[k]
            for j in range(k+1,SUB):
                for i in range(j,SUB):
                    A[i,j]=A[i,j]-M[i,k]*A[j,k] if i!=j else A[i,j]-M[i,k]*A[i,k]
        N={}
        for j in range(SUB):
            for i in range(j+1,SUB):
                s=M[i,j]
                for k in range(j+1,i):
                    s=s+M[i,k]*N[k,j]
                N[i,j]=-s
        dp=jnp.where(inb, jnp.where(lane-c0==sub,1.0,0.0), d)
        drow=[B(dp[j:j+1]) for j in range(SUB)]
        ncol=[]
        for j in range(SUB-1):
            m=jnp.zeros((SUB,TILE),jnp.float32)
            for i in range(j+1,SUB):
                m=jnp.where(sub==i,N[i,j],m)
            ncol.append(m)
        u=tree([dp]+[ncol[j]*drow[j] for j in range(SUB-1)])
        dvec=dd[0]
        for i in range(1,SUB):
            dvec=jnp.where(sub==i,dd[i],dvec)
        out.append(jnp.where(lane<c0+SUB,u*lax.rsqrt(dvec),0.0))
        if g==n-1: break
        ub=[B(u[i:i+1])*r[i] for i in range(SUB)]
        Z=[tree([ub[j]]+[N[i,j]*ub[i] for i in range(j+1,SUB)]) for j in range(SUB)]
        for t in range(g+1,n):
            cb=[B(rows[t][:,c0+j:c0+j+1]) for j in range(SUB)]
            rows[t]=jnp.where(inb,0.0,rows[t])-tree([cb[j]*Z[j] for j in range(SUB)])
    return jnp.concatenate(out,axis=0)

def factor_kernel(a_ref, b_ref, inv_ref, t_ref):
    t_ref[...] = jnp.zeros_like(t_ref)
    for n, (j, k) in enumerate(UPPER):
        t_ref[j * TILE : (j + 1) * TILE, k * TILE : (k + 1) * TILE] = a_ref[n] + b_ref[n]
    eye = (
        lax.broadcasted_iota(jnp.int32, (TILE, TILE), 0)
        == lax.broadcasted_iota(jnp.int32, (TILE, TILE), 1)
    ).astype(jnp.float32)
    for j in range(TILES):
        t_ref[j * TILE : (j + 1) * TILE, PANEL + j * TILE : PANEL + (j + 1) * TILE] = eye

    @pl.loop(0, TILES)
    def _(j):
        here = pl.ds(pl.multiple_of(j * TILE, TILE), TILE)
        inv = inverse_factor(t_ref[here, here])
        scaled = jnp.dot(
            inv, t_ref[here, :], precision=lax.Precision.HIGHEST, preferred_element_type=jnp.float32
        )
        inv_ref[here, :] = scaled[:, PANEL:]
        lane = lax.broadcasted_iota(jnp.int32, (TILE, PANEL), 1)
        ahead = jnp.where(lane >= (j + 1) * TILE, scaled[:, :PANEL], 0.0).T
        for i in range(1, TILES):

            @pl.when(i > j)
            def _():
                part = slice(i * TILE, (i + 1) * TILE)
                t_ref[part, :] -= jnp.dot(
                    ahead[part],
                    scaled,
                    precision=lax.Precision.HIGHEST,
                    preferred_element_type=jnp.float32,
                )


def inverse_of_factor(mine, other):
    return pl.pallas_call(
        factor_kernel,
        out_shape=jax.ShapeDtypeStruct((PANEL, PANEL), jnp.float32),
        in_specs=[pl.BlockSpec(memory_space=pltpu.VMEM)] * 2,
        out_specs=pl.BlockSpec(memory_space=pltpu.VMEM),
        scratch_shapes=[pltpu.VMEM((PANEL, 2 * PANEL), jnp.float32)],
        cost_estimate=pl.CostEstimate(
            flops=2 * 10**10, bytes_accessed=3 * 10**6, transcendentals=PANEL
        ),
        name="factor",
    )(mine, other)


def general_body(border, barrier, row_counts):
    scen_here, capacity, own_cols = border.shape
    n_scen = lax.axis_size("scen")
    per_owner = PANEL // lax.axis_size("col")
    rows_owned = own_cols // n_scen
    depth = scen_here * capacity
    positions = lax.iota(jnp.int32, capacity)
    weights = jnp.where(positions[None, :] < row_counts[:, None], 1.0 / barrier, jnp.float32(0.0))
    panel_part = jnp.transpose(border[:, :, :per_owner], (2, 0, 1)).reshape(per_owner, depth)
    panel = lax.all_gather(panel_part, "col", axis=0, tiled=True)
    weighted = panel * weights.reshape(1, depth)
    block = jnp.einsum(
        "pr,qr->pq", weighted, panel, precision=lax.Precision.HIGH,
        preferred_element_type=jnp.float32,
    )
    upper = jnp.stack(
        [block[j * TILE : (j + 1) * TILE, k * TILE : (k + 1) * TILE] for j, k in UPPER]
    )
    if n_scen == 2:
        swap = [(0, 1), (1, 0)]
        upper_other = lax.ppermute(upper, "scen", swap)
    else:
        upper_other = lax.psum(upper, "scen") - upper
    part = jnp.einsum(
        "pr,rc->pc", weighted, border.reshape(depth, own_cols), precision=lax.Precision.HIGH,
        preferred_element_type=jnp.float32,
    )
    if n_scen == 2:
        me = lax.axis_index("scen")
        sent = lax.dynamic_slice_in_dim(part, (1 - me) * rows_owned, rows_owned, 1)
        kept = lax.dynamic_slice_in_dim(part, me * rows_owned, rows_owned, 1)
        owned = kept + lax.ppermute(sent, "scen", swap)
    else:
        owned = lax.psum_scatter(part, "scen", scatter_dimension=1, tiled=True)
    inverse = inverse_of_factor(upper, upper_other)
    solved = jnp.einsum(
        "qt,pq->tp", owned, inverse, precision=lax.Precision.HIGHEST,
        preferred_element_type=jnp.float32,
    )
    return solved.reshape(1, 1, rows_owned, PANEL)


MESH = pl.DeviceIdType.MESH
CHUNK = 256
LAG = 3


def split(x):
    hi = x.astype(jnp.bfloat16)
    return hi, (x - hi.astype(jnp.float32)).astype(jnp.bfloat16)


def exact(a, b):
    return jnp.dot(a, b, precision=lax.Precision.HIGHEST, preferred_element_type=jnp.float32)


def bf16_nt(a, b):
    return lax.dot_general(a, b, (((1,), (1,)), ((), ())), preferred_element_type=jnp.float32)


def bf16_nn(a, b):
    return jnp.dot(a, b, preferred_element_type=jnp.float32)


def ring_kernel(
    barrier_ref, counts_ref, border_ref, out_ref,
    pan, part_ref, w_ref, gath, stage, bhi, blo, phi, plo, whi, wlo,
    u_keep, u_send, u_recv, g_own, g_recv, t_ref, inv_ref, low_ref, x_ref,
    pan_sem, stage_sem, ring_send, core_send, recv_sem, uy_send, uy_recv, gy_send, gy_recv,
):
    chips = lax.axis_size("col") // 2
    half_ring = chips // 2
    me = lax.axis_index("col")
    scen = lax.axis_index("scen")
    core = me % 2
    chip = me // 2
    pos = (1 - chip % 2) * (chip // 2) + (chip % 2) * (chips - 1 - chip // 2)
    depth_half = part_ref.shape[2]
    per = part_ref.shape[1]
    depth = 2 * depth_half
    cols = border_ref.shape[1]
    rows_owned = cols // 2

    def chip_at(p):
        p = (p + 2 * chips) % chips
        x = p // half_ring
        z = (1 - x) * p + x * (chips - 1 - p)
        return 2 * z + x

    up = {"col": 2 * chip_at(pos + 1) + core}
    down = {"col": 2 * chip_at(pos - 1) + core}
    mate = {"col": 2 * chip + 1 - core}
    across = {"scen": 1 - scen}

    barrier = pltpu.get_barrier_semaphore()
    for peer in (up, down, mate, across):
        pl.semaphore_signal(barrier, inc=1, device_id=peer, device_id_type=MESH)

    def fetch(n):
        return pltpu.make_async_copy(
            border_ref.at[pl.ds(pl.multiple_of(n * CHUNK, CHUNK), CHUNK)],
            stage.at[n % LAG],
            stage_sem.at[n % LAG],
        )

    def fetch_panel(h):
        return pltpu.make_async_copy(
            border_ref.at[pl.ds(h * depth_half, depth_half), pl.ds(0, TILE)],
            pan.at[h],
            pan_sem.at[h],
        )

    chunks = depth // CHUNK
    for h in range(2):
        fetch_panel(h).start()
    for n in range(LAG):
        fetch(n).start()

    def send(src, block, h, send_sem, peer):
        return pltpu.make_async_remote_copy(
            src_ref=src,
            dst_ref=gath.at[block, h],
            send_sem=send_sem,
            recv_sem=recv_sem.at[block, h],
            device_id=peer,
            device_id_type=MESH,
        )

    def own(h, d):
        sem = core_send.at[0, h] if d == 2 else ring_send.at[d, 0, h]
        return send(part_ref.at[h], me, h, sem, (up, down, mate)[d])

    def block_of(d, k):
        return 2 * chip_at(pos - k if d == 0 else pos + k) + core

    def forward(d, k, h):
        block = block_of(d, k)
        return send(gath.at[block, h], block, h, ring_send.at[d, k, h], (up, down)[d])

    def push(d, k, h):
        block = block_of(d, k)
        return send(gath.at[block, h], block, h, core_send.at[2 * k - d, h], mate)

    def arrived(block, h):
        pltpu.make_async_copy(part_ref.at[h], gath.at[block, h], recv_sem.at[block, h]).wait()

    for h in range(2):
        fetch_panel(h).wait()
        for n in range(depth_half // TILE):
            here = slice(n * TILE, (n + 1) * TILE)
            part_ref[h, :, here] = pan[h, here, :].T[:per]
        if h == 0:
            pl.semaphore_wait(barrier, 4)
        for d in range(3):
            own(h, d).start()
    place = lax.broadcasted_iota(jnp.int32, (1, depth_half), 1)
    for h in range(2):
        w_ref[h : h + 1, :] = jnp.where(place < counts_ref[h], 1.0 / barrier_ref[h : h + 1, :], 0.0)

    def convert_border(first):
        @pl.loop(first, first + chunks // 2)
        def _(n):
            fetch(n).wait()
            here = pl.ds(pl.multiple_of(n * CHUNK, CHUNK), CHUNK)
            hi, lo = split(stage[n % LAG])
            bhi[here, :] = hi
            blo[here, :] = lo

            @pl.when(n + LAG < chunks)
            def _():
                fetch(n + LAG).start()

    def convert(which, cc, src):
        for h in range(2):
            there = (which, pl.ds(cc * per, per), pl.ds(h * depth_half, depth_half))
            x = src(h)
            phi[there], plo[there] = split(x)
            whi[there], wlo[there] = split(x * w_ref[h : h + 1, :])

    def convert_both(which):
        for cc in range(2):
            convert(which, cc, lambda h: gath[2 * which + cc, h])

    def product(unit, which, dst):
        left = jnp.concatenate([ref[a] for ref in (whi, wlo) for a in unit], axis=0)
        rows = left.shape[0] // 2
        each = whi.shape[1]

        @pl.loop(0, rows_owned // CHUNK)
        def _(n):
            col = pl.ds(pl.multiple_of(which * rows_owned + n * CHUNK, CHUNK), CHUNK)
            to = pl.ds(pl.multiple_of(n * CHUNK, CHUNK), CHUNK)
            both = bf16_nn(left, bhi[:, col])
            res = both[:rows] + both[rows:] + bf16_nn(left[:rows], blo[:, col])
            for n, a in enumerate(unit):
                dst[a, :, to] = res[n * each : (n + 1) * each]

    def cross(which):
        return pltpu.make_async_remote_copy(
            src_ref=u_send.at[which],
            dst_ref=u_recv.at[which],
            send_sem=uy_send.at[which],
            recv_sem=uy_recv.at[which],
            device_id=across,
            device_id_type=MESH,
        )

    def product_send(unit):
        product(unit, 1 - scen, u_send)
        for which in unit:
            cross(which).start()

    def g_piece(n):
        row = max(n - 1, 0)
        first, last = (0, TILE) if n == 0 else (max(row, 1) * TILE, PANEL)
        at = (row, slice(None), slice(first, last))
        return pltpu.make_async_remote_copy(
            src_ref=g_own.at[at],
            dst_ref=g_recv.at[at],
            send_sem=gy_send.at[n],
            recv_sem=gy_recv.at[n],
            device_id=across,
            device_id_type=MESH,
        )

    def gram(i):
        pair = 2 * i
        rows = TILE
        left = jnp.concatenate([whi[pair], whi[pair + 1], wlo[pair], wlo[pair + 1]], axis=0)
        count = 2 * (TILES - i)
        right_hi = phi[pair : pair + count].reshape(count * 2 * per, depth)
        right_lo = plo[pair : pair + count].reshape(count * 2 * per, depth)
        both = bf16_nt(left, right_hi)
        res = both[:rows] + both[rows:] + bf16_nt(left[:rows], right_lo)
        g_own[i, :, i * TILE :] = res
        t_ref[i * TILE : (i + 1) * TILE, i * TILE :] = res

    def receive(d, k, h, first):
        block = block_of(d, k)
        arrived(block, h)
        push(d, k, h).start()

        @pl.when(k < half_ring - 1 + first)
        def _():
            forward(d, k, h).start()

    @pl.loop(1, half_ring)
    def _(k):
        @pl.when(k == 1)
        def _():
            convert_border(0)

        receive(0, k, 0, 1)
        receive(1, k, 0, 0)

        @pl.when(k == 1)
        def _():
            convert_border(chunks // 2)
            for h in range(2):
                arrived(2 * chip + 1 - core, h)
            convert(chip, core, lambda h: part_ref[h])
            convert(chip, 1 - core, lambda h: gath[2 * chip + 1 - core, h])
            product_send([chip])

        before = [chip_at(pos - k + 1), chip_at(pos + k - 1)]

        @pl.when(k > 1)
        def _():
            product_send(before)

        receive(1, k, 1, 1)
        receive(0, k, 1, 0)

        @pl.when(k == 1)
        def _():
            product([chip], scen, u_keep)

        @pl.when(k > 1)
        def _():
            product(before, scen, u_keep)

        for d in range(2):
            which = block_of(d, k) // 2
            for h in range(2):
                arrived(2 * which + 1 - core, h)
            convert_both(which)

    last = [chip_at(pos - half_ring + 1), chip_at(pos + half_ring - 1)]
    far = chip_at(pos + half_ring)
    product_send(last)
    for h in range(2):
        arrived(block_of(h, half_ring), h)
        push(h, half_ring, h).start()
    product(last, scen, u_keep)
    for h in range(2):
        arrived(2 * far + 1 - core, h)
    convert_both(far)
    for i in range(TILES):
        gram(i)
        if i == 0:
            g_piece(0).start()
        g_piece(i + 1).start()
    product_send([far])
    product([far], scen, u_keep)

    def tiles(i):
        return slice(i * TILE, (i + 1) * TILE)

    g_piece(0).wait_recv()
    t_ref[:TILE, :TILE] += g_recv[0, :, :TILE]
    inv = inverse_factor(t_ref[:TILE, :TILE])
    g_piece(1).wait_recv()
    t_ref[:TILE, TILE:] += g_recv[0, :, TILE:]
    for j in range(TILES):
        inv_ref[j] = inv
        if j == TILES - 1:
            break
        scaled = exact(inv, t_ref[tiles(j), (j + 1) * TILE :])
        ahead = scaled.T
        low_ref[(j + 1) * TILE :, tiles(j)] = ahead
        g_piece(j + 2).wait_recv()
        t_ref[tiles(j + 1), (j + 1) * TILE :] += g_recv[j + 1, :, (j + 1) * TILE :]
        if j == TILES - 2:
            for which in range(chips):
                cross(which).wait_recv()
        pivot = t_ref[tiles(j + 1), tiles(j + 1)] - exact(ahead[:TILE], scaled[:, :TILE])
        inv = inverse_factor(pivot)
        for i in range(j + 1, TILES):
            first = max(i, j + 2)
            if first < TILES:
                t_ref[tiles(i), first * TILE :] -= exact(
                    ahead[tiles(i - j - 1)], scaled[:, (first - j - 1) * TILE :]
                )
        if j == TILES - 2:
            for i in range(TILES):
                pair = slice(2 * i, 2 * i + 2)
                x_ref[tiles(i), :] = (u_keep[pair] + u_recv[pair]).reshape(TILE, rows_owned)
            for i in range(TILES - 1):
                x = exact(inv_ref[i], x_ref[tiles(i), :])
                out_ref[:, tiles(i)] = x.T
                x_ref[(i + 1) * TILE :, :] -= exact(low_ref[(i + 1) * TILE :, tiles(i)], x)
    out_ref[:, tiles(TILES - 1)] = exact(inv, x_ref[tiles(TILES - 1), :]).T

    for h in range(2):
        for d in range(3):
            own(h, d).wait_send()
    for k in range(1, half_ring + 1):
        for d in range(2):
            for h in range(2):
                if k < half_ring - 1 or (k < half_ring and d == h):
                    forward(d, k, h).wait_send()
                if k < half_ring or d == h:
                    push(d, k, h).wait_send()
    for which in range(chips):
        cross(which).wait_send()
    for n in range(TILES + 1):
        g_piece(n).wait_send()


def ring_body(border, barrier, row_counts):
    scen_here, capacity, own_cols = border.shape
    n_col = lax.axis_size("col")
    chips = n_col // 2
    per = PANEL // n_col
    depth = scen_here * capacity
    rows_owned = own_cols // lax.axis_size("scen")
    dma = pltpu.SemaphoreType.DMA
    f32, bf16 = jnp.float32, jnp.bfloat16
    solved = pl.pallas_call(
        ring_kernel,
        out_shape=jax.ShapeDtypeStruct((rows_owned, PANEL), f32),
        in_specs=[
            pl.BlockSpec(memory_space=pltpu.VMEM),
            pl.BlockSpec(memory_space=pltpu.SMEM),
            pl.BlockSpec(memory_space=pl.ANY),
        ],
        out_specs=pl.BlockSpec(memory_space=pltpu.VMEM),
        scratch_shapes=[
            pltpu.VMEM((scen_here, capacity, TILE), f32),
            pltpu.VMEM((scen_here, per, capacity), f32),
            pltpu.VMEM((scen_here, capacity), f32),
            pltpu.VMEM((n_col, scen_here, per, capacity), f32),
            pltpu.VMEM((LAG, CHUNK, own_cols), f32),
            pltpu.VMEM((depth, own_cols), bf16),
            pltpu.VMEM((depth, own_cols), bf16),
            *[pltpu.VMEM((chips, 2 * per, depth), bf16)] * 4,
            *[pltpu.VMEM((chips, 2 * per, rows_owned), f32)] * 3,
            *[pltpu.VMEM((TILES, TILE, PANEL), f32)] * 2,
            pltpu.VMEM((PANEL, PANEL), f32),
            pltpu.VMEM((TILES, TILE, TILE), f32),
            pltpu.VMEM((PANEL, PANEL), f32),
            pltpu.VMEM((PANEL, rows_owned), f32),
            dma((scen_here,)),
            dma((LAG,)),
            dma((2, chips // 2, 2)),
            dma((chips + 1, 2)),
            dma((n_col, 2)),
            dma((chips,)),
            dma((chips,)),
            dma((TILES + 1,)),
            dma((TILES + 1,)),
        ],
        compiler_params=pltpu.CompilerParams(
            collective_id=0, has_side_effects=True, vmem_limit_bytes=60 * 2**20
        ),
        name="ring",
    )(barrier, row_counts, border.reshape(depth, own_cols))
    return solved.reshape(1, 1, rows_owned, PANEL)


def solution(mesh):
    n_scen, n_col = mesh.shape["scen"], mesh.shape["col"]
    ring = n_scen == 2 and 4 * (PANEL // n_col) == TILE
    placed = (P("scen", None, "col"), P("scen", None), P("scen"))
    return jax.shard_map(
        ring_body if ring else general_body,
        mesh=mesh,
        in_specs=placed,
        out_specs=P("col", "scen", None, None),
        check_vma=False,
    )
```

```python
import jax
import jax.numpy as jnp
from jax import lax
from jax.experimental import pallas as pl
from jax.experimental.pallas import tpu as pltpu
from jax.sharding import PartitionSpec as P

PANEL = 512
TILE = 128
SUB = 8
TILES = PANEL // TILE
UPPER = [(j, k) for j in range(TILES) for k in range(j, TILES)]


def tree(xs):
    xs=list(xs)
    while len(xs)>1:
        xs=[xs[i]+xs[i+1] if i+1<len(xs) else xs[i] for i in range(0,len(xs),2)]
    return xs[0]

def lane_of(x, c):
    return jnp.take_along_axis(x, jnp.full((SUB, TILE), c, jnp.int32), axis=1)


def row_of(x, i):
    return jnp.take_along_axis(x, jnp.full((SUB, TILE), i, jnp.int32), axis=0)


def inverse_factor(a):
    n = TILE // SUB
    lane = lax.broadcasted_iota(jnp.int32, (SUB, TILE), 1)
    sub = lax.broadcasted_iota(jnp.int32, (SUB, TILE), 0)
    rows = [a[SUB * t : SUB * (t + 1)] for t in range(n)]
    out = []
    each = range(SUB)
    for g in range(n):
        c0 = g * SUB
        d = rows[g]
        inside = (lane >= c0) & (lane < c0 + SUB)
        cols = [lane_of(d, c0 + j) for j in each]
        s = {(i, j): row_of(cols[j], i) for j in each for i in range(j, SUB)}
        mixed = jnp.where(inside, jnp.where(lane - c0 == sub, 1.0, 0.0), d)
        u = [row_of(mixed, i) for i in each]
        more = g + 1 < n
        if more:
            below = [lane_of(rows[g + 1], c0 + j) for j in each]
            ahead = jnp.where(inside, 0.0, rows[g + 1])
        m, ur = {}, []
        for k in each:
            r = 1.0 / s[k, k]
            for i in range(k + 1, SUB):
                m[i, k] = s[i, k] * r
            for j in range(k + 1, SUB):
                for i in range(j, SUB):
                    s[i, j] = s[i, j] - m[i, k] * s[j, k]
            ur.append(u[k] * r)
            for i in range(k + 1, SUB):
                u[i] = u[i] - m[i, k] * u[k]
            if more:
                for i in range(k + 1, SUB):
                    below[i] = below[i] - m[i, k] * below[k]
                ahead = ahead - below[k] * ur[k]
        whole, pivot = u[0], s[0, 0]
        for i in range(1, SUB):
            whole = jnp.where(sub == i, u[i], whole)
            pivot = jnp.where(sub == i, s[i, i], pivot)
        out.append(jnp.where(lane < c0 + SUB, whole * lax.rsqrt(pivot), 0.0))
        if not more:
            break
        rows[g + 1] = ahead
        z = [None] * SUB
        for j in reversed(each):
            z[j] = ur[j]
            for i in range(j + 1, SUB):
                z[j] = z[j] - m[i, j] * z[i]
        for t in range(g + 2, n):
            terms = [lane_of(rows[t], c0 + j) * z[j] for j in each]
            rows[t] = jnp.where(inside, 0.0, rows[t]) - tree(terms)
    return jnp.concatenate(out, axis=0)


def factor_kernel(a_ref, b_ref, inv_ref, t_ref):
    t_ref[...] = jnp.zeros_like(t_ref)
    for n, (j, k) in enumerate(UPPER):
        t_ref[j * TILE : (j + 1) * TILE, k * TILE : (k + 1) * TILE] = a_ref[n] + b_ref[n]
    eye = (
        lax.broadcasted_iota(jnp.int32, (TILE, TILE), 0)
        == lax.broadcasted_iota(jnp.int32, (TILE, TILE), 1)
    ).astype(jnp.float32)
    for j in range(TILES):
        t_ref[j * TILE : (j + 1) * TILE, PANEL + j * TILE : PANEL + (j + 1) * TILE] = eye

    @pl.loop(0, TILES)
    def _(j):
        here = pl.ds(pl.multiple_of(j * TILE, TILE), TILE)
        inv = inverse_factor(t_ref[here, here])
        scaled = jnp.dot(
            inv, t_ref[here, :], precision=lax.Precision.HIGHEST, preferred_element_type=jnp.float32
        )
        inv_ref[here, :] = scaled[:, PANEL:]
        lane = lax.broadcasted_iota(jnp.int32, (TILE, PANEL), 1)
        ahead = jnp.where(lane >= (j + 1) * TILE, scaled[:, :PANEL], 0.0).T
        for i in range(1, TILES):

            @pl.when(i > j)
            def _():
                part = slice(i * TILE, (i + 1) * TILE)
                t_ref[part, :] -= jnp.dot(
                    ahead[part],
                    scaled,
                    precision=lax.Precision.HIGHEST,
                    preferred_element_type=jnp.float32,
                )


def inverse_of_factor(mine, other):
    return pl.pallas_call(
        factor_kernel,
        out_shape=jax.ShapeDtypeStruct((PANEL, PANEL), jnp.float32),
        in_specs=[pl.BlockSpec(memory_space=pltpu.VMEM)] * 2,
        out_specs=pl.BlockSpec(memory_space=pltpu.VMEM),
        scratch_shapes=[pltpu.VMEM((PANEL, 2 * PANEL), jnp.float32)],
        cost_estimate=pl.CostEstimate(
            flops=2 * 10**10, bytes_accessed=3 * 10**6, transcendentals=PANEL
        ),
        name="factor",
    )(mine, other)


def general_body(border, barrier, row_counts):
    scen_here, capacity, own_cols = border.shape
    n_scen = lax.axis_size("scen")
    per_owner = PANEL // lax.axis_size("col")
    rows_owned = own_cols // n_scen
    depth = scen_here * capacity
    positions = lax.iota(jnp.int32, capacity)
    weights = jnp.where(positions[None, :] < row_counts[:, None], 1.0 / barrier, jnp.float32(0.0))
    panel_part = jnp.transpose(border[:, :, :per_owner], (2, 0, 1)).reshape(per_owner, depth)
    panel = lax.all_gather(panel_part, "col", axis=0, tiled=True)
    weighted = panel * weights.reshape(1, depth)
    block = jnp.einsum(
        "pr,qr->pq", weighted, panel, precision=lax.Precision.HIGH,
        preferred_element_type=jnp.float32,
    )
    upper = jnp.stack(
        [block[j * TILE : (j + 1) * TILE, k * TILE : (k + 1) * TILE] for j, k in UPPER]
    )
    if n_scen == 2:
        swap = [(0, 1), (1, 0)]
        upper_other = lax.ppermute(upper, "scen", swap)
    else:
        upper_other = lax.psum(upper, "scen") - upper
    part = jnp.einsum(
        "pr,rc->pc", weighted, border.reshape(depth, own_cols), precision=lax.Precision.HIGH,
        preferred_element_type=jnp.float32,
    )
    if n_scen == 2:
        me = lax.axis_index("scen")
        sent = lax.dynamic_slice_in_dim(part, (1 - me) * rows_owned, rows_owned, 1)
        kept = lax.dynamic_slice_in_dim(part, me * rows_owned, rows_owned, 1)
        owned = kept + lax.ppermute(sent, "scen", swap)
    else:
        owned = lax.psum_scatter(part, "scen", scatter_dimension=1, tiled=True)
    inverse = inverse_of_factor(upper, upper_other)
    solved = jnp.einsum(
        "qt,pq->tp", owned, inverse, precision=lax.Precision.HIGHEST,
        preferred_element_type=jnp.float32,
    )
    return solved.reshape(1, 1, rows_owned, PANEL)


MESH = pl.DeviceIdType.MESH
CHUNK = 256
LAG = 3


def split(x):
    hi = x.astype(jnp.bfloat16)
    return hi, (x - hi.astype(jnp.float32)).astype(jnp.bfloat16)


def exact(a, b):
    return jnp.dot(a, b, precision=lax.Precision.HIGHEST, preferred_element_type=jnp.float32)


def bf16_nt(a, b):
    return lax.dot_general(a, b, (((1,), (1,)), ((), ())), preferred_element_type=jnp.float32)


def bf16_nn(a, b):
    return jnp.dot(a, b, preferred_element_type=jnp.float32)


def ring_kernel(
    barrier_ref, counts_ref, border_ref, out_ref,
    pan, part_ref, w_ref, gath, stage, bhi, blo, phi, plo, whi, wlo,
    u_keep, u_send, u_recv, g_own, g_recv, t_ref, inv_ref, low_ref, x_ref,
    pan_sem, stage_sem, ring_send, core_send, recv_sem, uy_send, uy_recv, gy_send, gy_recv, g_push_sem,
):
    chips = lax.axis_size("col") // 2
    half_ring = chips // 2
    me = lax.axis_index("col")
    scen = lax.axis_index("scen")
    core = me % 2
    chip = me // 2
    pos = (1 - chip % 2) * (chip // 2) + (chip % 2) * (chips - 1 - chip // 2)
    depth_half = part_ref.shape[2]
    per = part_ref.shape[1]
    depth = 2 * depth_half
    cols = border_ref.shape[1]
    rows_owned = cols // 2

    def chip_at(p):
        p = (p + 2 * chips) % chips
        x = p // half_ring
        z = (1 - x) * p + x * (chips - 1 - p)
        return 2 * z + x

    up = {"col": 2 * chip_at(pos + 1) + core}
    down = {"col": 2 * chip_at(pos - 1) + core}
    mate = {"col": 2 * chip + 1 - core}
    across = {"scen": 1 - scen}

    barrier = pltpu.get_barrier_semaphore()
    for peer in (up, down, mate, across):
        pl.semaphore_signal(barrier, inc=1, device_id=peer, device_id_type=MESH)

    def fetch(n):
        return pltpu.make_async_copy(
            border_ref.at[pl.ds(pl.multiple_of(n * CHUNK, CHUNK), CHUNK)],
            stage.at[n % LAG],
            stage_sem.at[n % LAG],
        )

    def fetch_panel(h):
        return pltpu.make_async_copy(
            border_ref.at[pl.ds(h * depth_half, depth_half), pl.ds(0, TILE)],
            pan.at[h],
            pan_sem.at[h],
        )

    chunks = depth // CHUNK
    for h in range(2):
        fetch_panel(h).start()
    for n in range(LAG):
        fetch(n).start()

    def send(src, block, h, send_sem, peer):
        return pltpu.make_async_remote_copy(
            src_ref=src,
            dst_ref=gath.at[block, h],
            send_sem=send_sem,
            recv_sem=recv_sem.at[block, h],
            device_id=peer,
            device_id_type=MESH,
        )

    def own(h, d):
        sem = core_send.at[0, h] if d == 2 else ring_send.at[d, 0, h]
        return send(part_ref.at[h], me, h, sem, (up, down, mate)[d])

    def block_of(d, k):
        return 2 * chip_at(pos - k if d == 0 else pos + k) + core

    def forward(d, k, h):
        block = block_of(d, k)
        return send(gath.at[block, h], block, h, ring_send.at[d, k, h], (up, down)[d])

    def push(d, k, h):
        block = block_of(d, k)
        return send(gath.at[block, h], block, h, core_send.at[2 * k - d, h], mate)

    def arrived(block, h):
        pltpu.make_async_copy(part_ref.at[h], gath.at[block, h], recv_sem.at[block, h]).wait()

    for h in range(2):
        fetch_panel(h).wait()
        for n in range(depth_half // TILE):
            here = slice(n * TILE, (n + 1) * TILE)
            part_ref[h, :, here] = pan[h, here, :].T[:per]
        if h == 0:
            pl.semaphore_wait(barrier, 4)
        for d in range(3):
            own(h, d).start()
    place = lax.broadcasted_iota(jnp.int32, (1, depth_half), 1)
    for h in range(2):
        w_ref[h : h + 1, :] = jnp.where(place < counts_ref[h], 1.0 / barrier_ref[h : h + 1, :], 0.0)

    def convert_border(first):
        @pl.loop(first, first + chunks // 2)
        def _(n):
            fetch(n).wait()
            here = pl.ds(pl.multiple_of(n * CHUNK, CHUNK), CHUNK)
            hi, lo = split(stage[n % LAG])
            bhi[here, :] = hi
            blo[here, :] = lo

            @pl.when(n + LAG < chunks)
            def _():
                fetch(n + LAG).start()

    def convert(which, cc, src):
        for h in range(2):
            there = (which, pl.ds(cc * per, per), pl.ds(h * depth_half, depth_half))
            x = src(h)
            phi[there], plo[there] = split(x)
            whi[there], wlo[there] = split(x * w_ref[h : h + 1, :])

    def convert_both(which):
        for cc in range(2):
            convert(which, cc, lambda h: gath[2 * which + cc, h])

    def product(unit, which, dst, unroll=False):
        left = jnp.concatenate([ref[a] for ref in (whi, wlo) for a in unit], axis=0)
        rows = left.shape[0] // 2
        each = whi.shape[1]

        def columns(n):
            col = pl.ds(pl.multiple_of(which * rows_owned + n * CHUNK, CHUNK), CHUNK)
            to = pl.ds(pl.multiple_of(n * CHUNK, CHUNK), CHUNK)
            both = bf16_nn(left, bhi[:, col])
            res = both[:rows] + both[rows:] + bf16_nn(left[:rows], blo[:, col])
            for i, a in enumerate(unit):
                dst[a, :, to] = res[i * each : (i + 1) * each]

        if unroll:
            for n in range(rows_owned // CHUNK):
                columns(n)
        else:
            pl.loop(0, rows_owned // CHUNK)(columns)

    def cross(which):
        return pltpu.make_async_remote_copy(
            src_ref=u_send.at[which],
            dst_ref=u_recv.at[which],
            send_sem=uy_send.at[which],
            recv_sem=uy_recv.at[which],
            device_id=across,
            device_id_type=MESH,
        )

    def product_send(unit, unroll=False):
        product(unit, 1 - scen, u_send, unroll)
        for which in unit:
            cross(which).start()

    def g_at(n):
        row = max(n - 1, 0)
        first, last = (0, TILE) if n == 0 else (max(row, 1) * TILE, PANEL)
        return row, slice(None), slice(first, last)

    def g_owner(n):
        return (n // 2) % 2

    def g_start(n):
        @pl.when(core == g_owner(n))
        def _():
            g_piece(n).start()

    def g_push(n):
        return pltpu.make_async_remote_copy(
            src_ref=g_recv.at[g_at(n)],
            dst_ref=g_recv.at[g_at(n)],
            send_sem=g_push_sem.at[n],
            recv_sem=gy_recv.at[n],
            device_id=mate,
            device_id_type=MESH,
        )

    def g_relay(n):
        @pl.when(core == g_owner(n))
        def _():
            g_piece(n).wait_recv()
            g_push(n).start()

    def g_wait(n):
        @pl.when(core != g_owner(n))
        def _():
            g_piece(n).wait_recv()

    def g_piece(n):
        at = g_at(n)
        return pltpu.make_async_remote_copy(
            src_ref=g_own.at[at],
            dst_ref=g_recv.at[at],
            send_sem=gy_send.at[n],
            recv_sem=gy_recv.at[n],
            device_id=across,
            device_id_type=MESH,
        )

    def gram(i):
        pair = 2 * i
        rows = TILE
        left = jnp.concatenate([whi[pair], whi[pair + 1], wlo[pair], wlo[pair + 1]], axis=0)
        count = 2 * (TILES - i)
        right_hi = phi[pair : pair + count].reshape(count * 2 * per, depth)
        right_lo = plo[pair : pair + count].reshape(count * 2 * per, depth)
        both = bf16_nt(left, right_hi)
        res = both[:rows] + both[rows:] + bf16_nt(left[:rows], right_lo)
        g_own[i, :, i * TILE :] = res
        t_ref[i * TILE : (i + 1) * TILE, i * TILE :] = res

    def receive(d, k, h, first):
        block = block_of(d, k)
        arrived(block, h)
        push(d, k, h).start()

        @pl.when(k < half_ring - 1 + first)
        def _():
            forward(d, k, h).start()

    @pl.loop(1, half_ring)
    def _(k):
        @pl.when(k == 1)
        def _():
            convert_border(0)

        receive(0, k, 0, 1)
        receive(1, k, 0, 0)

        @pl.when(k == 1)
        def _():
            convert_border(chunks // 2)
            for h in range(2):
                arrived(2 * chip + 1 - core, h)
            convert(chip, core, lambda h: part_ref[h])
            convert(chip, 1 - core, lambda h: gath[2 * chip + 1 - core, h])
            product_send([chip])

        before = [chip_at(pos - k + 1), chip_at(pos + k - 1)]

        @pl.when(k > 1)
        def _():
            product_send(before)

        receive(1, k, 1, 1)
        receive(0, k, 1, 0)

        @pl.when(k == 1)
        def _():
            product([chip], scen, u_keep)

        @pl.when(k > 1)
        def _():
            product(before, scen, u_keep)

        for d in range(2):
            which = block_of(d, k) // 2
            for h in range(2):
                arrived(2 * which + 1 - core, h)
            convert_both(which)

    last = [chip_at(pos - half_ring + 1), chip_at(pos + half_ring - 1)]
    far = chip_at(pos + half_ring)
    product_send(last)
    for h in range(2):
        arrived(block_of(h, half_ring), h)
        push(h, half_ring, h).start()
    product(last, scen, u_keep)
    for h in range(2):
        arrived(2 * far + 1 - core, h)
    convert_both(far)
    gram(0)
    g_piece(0).start()
    g_start(1)
    for i in range(1, TILES):
        gram(i)
        g_start(i + 1)

    def tiles(i):
        return slice(i * TILE, (i + 1) * TILE)

    g_piece(0).wait_recv()
    t_ref[:TILE, :TILE] += g_recv[0, :, :TILE]
    inv = inverse_factor(t_ref[:TILE, :TILE])
    product([far], 1 - scen, u_send, True)
    product([far], scen, u_keep, True)
    cross(far).start()
    g_relay(1)
    g_relay(2)
    g_wait(1)
    t_ref[:TILE, TILE:] += g_recv[0, :, TILE:]
    for j in range(TILES):
        inv_ref[j] = inv
        if j == TILES - 1:
            break
        if j == 1:
            g_relay(3)
            g_relay(4)
        scaled = exact(inv, t_ref[tiles(j), (j + 1) * TILE :])
        ahead = scaled.T
        low_ref[(j + 1) * TILE :, tiles(j)] = ahead
        g_wait(j + 2)
        t_ref[tiles(j + 1), (j + 1) * TILE :] += g_recv[j + 1, :, (j + 1) * TILE :]
        if j == TILES - 2:
            for which in range(chips):
                cross(which).wait_recv()
        pivot = t_ref[tiles(j + 1), tiles(j + 1)] - exact(ahead[:TILE], scaled[:, :TILE])
        inv = inverse_factor(pivot)
        for i in range(j + 1, TILES):
            first = max(i, j + 2)
            if first < TILES:
                t_ref[tiles(i), first * TILE :] -= exact(
                    ahead[tiles(i - j - 1)], scaled[:, (first - j - 1) * TILE :]
                )
        if j == TILES - 2:
            for i in range(TILES):
                pair = slice(2 * i, 2 * i + 2)
                x_ref[tiles(i), :] = (u_keep[pair] + u_recv[pair]).reshape(TILE, rows_owned)
            for i in range(TILES - 1):
                x = exact(inv_ref[i], x_ref[tiles(i), :])
                out_ref[:, tiles(i)] = x.T
                x_ref[(i + 1) * TILE :, :] -= exact(low_ref[(i + 1) * TILE :, tiles(i)], x)
    out_ref[:, tiles(TILES - 1)] = exact(inv, x_ref[tiles(TILES - 1), :]).T

    for h in range(2):
        for d in range(3):
            own(h, d).wait_send()
    for k in range(1, half_ring + 1):
        for d in range(2):
            for h in range(2):
                if k < half_ring - 1 or (k < half_ring and d == h):
                    forward(d, k, h).wait_send()
                if k < half_ring or d == h:
                    push(d, k, h).wait_send()
    for which in range(chips):
        cross(which).wait_send()
    g_piece(0).wait_send()
    for n in range(1, TILES + 1):

        @pl.when(core == g_owner(n))
        def _():
            g_piece(n).wait_send()
            g_push(n).wait_send()


def ring_body(border, barrier, row_counts):
    scen_here, capacity, own_cols = border.shape
    n_col = lax.axis_size("col")
    chips = n_col // 2
    per = PANEL // n_col
    depth = scen_here * capacity
    rows_owned = own_cols // lax.axis_size("scen")
    dma = pltpu.SemaphoreType.DMA
    f32, bf16 = jnp.float32, jnp.bfloat16
    solved = pl.pallas_call(
        ring_kernel,
        out_shape=jax.ShapeDtypeStruct((rows_owned, PANEL), f32),
        in_specs=[
            pl.BlockSpec(memory_space=pltpu.VMEM),
            pl.BlockSpec(memory_space=pltpu.SMEM),
            pl.BlockSpec(memory_space=pl.ANY),
        ],
        out_specs=pl.BlockSpec(memory_space=pltpu.VMEM),
        scratch_shapes=[
            pltpu.VMEM((scen_here, capacity, TILE), f32),
            pltpu.VMEM((scen_here, per, capacity), f32),
            pltpu.VMEM((scen_here, capacity), f32),
            pltpu.VMEM((n_col, scen_here, per, capacity), f32),
            pltpu.VMEM((LAG, CHUNK, own_cols), f32),
            pltpu.VMEM((depth, own_cols), bf16),
            pltpu.VMEM((depth, own_cols), bf16),
            *[pltpu.VMEM((chips, 2 * per, depth), bf16)] * 4,
            *[pltpu.VMEM((chips, 2 * per, rows_owned), f32)] * 3,
            *[pltpu.VMEM((TILES, TILE, PANEL), f32)] * 2,
            pltpu.VMEM((PANEL, PANEL), f32),
            pltpu.VMEM((TILES, TILE, TILE), f32),
            pltpu.VMEM((PANEL, PANEL), f32),
            pltpu.VMEM((PANEL, rows_owned), f32),
            dma((scen_here,)),
            dma((LAG,)),
            dma((2, chips // 2, 2)),
            dma((chips + 1, 2)),
            dma((n_col, 2)),
            dma((chips,)),
            dma((chips,)),
            dma((TILES + 1,)),
            dma((TILES + 1,)),
            dma((TILES + 1,)),
        ],
        compiler_params=pltpu.CompilerParams(
            collective_id=0, has_side_effects=True, vmem_limit_bytes=60 * 2**20
        ),
        name="ring",
    )(barrier, row_counts, border.reshape(depth, own_cols))
    return solved.reshape(1, 1, rows_owned, PANEL)


def solution(mesh):
    n_scen, n_col = mesh.shape["scen"], mesh.shape["col"]
    ring = n_scen == 2 and 4 * (PANEL // n_col) == TILE
    placed = (P("scen", None, "col"), P("scen", None), P("scen"))
    return jax.shard_map(
        ring_body if ring else general_body,
        mesh=mesh,
        in_specs=placed,
        out_specs=P("col", "scen", None, None),
        check_vma=False,
    )
```

```python
import jax
import jax.numpy as jnp
from jax import lax
from jax.experimental import pallas as pl
from jax.experimental.pallas import tpu as pltpu
from jax.sharding import PartitionSpec as P

PANEL = 512
TILE = 128
SUB = 8
TILES = PANEL // TILE
UPPER = [(j, k) for j in range(TILES) for k in range(j, TILES)]


def tree(xs):
    xs=list(xs)
    while len(xs)>1:
        xs=[xs[i]+xs[i+1] if i+1<len(xs) else xs[i] for i in range(0,len(xs),2)]
    return xs[0]

def lane_of(x, c):
    return jnp.take_along_axis(x, jnp.full((SUB, TILE), c, jnp.int32), axis=1)


def row_of(x, i):
    return jnp.take_along_axis(x, jnp.full((SUB, TILE), i, jnp.int32), axis=0)


def inverse_factor(a):
    n = TILE // SUB
    lane = lax.broadcasted_iota(jnp.int32, (SUB, TILE), 1)
    sub = lax.broadcasted_iota(jnp.int32, (SUB, TILE), 0)
    rows = [a[SUB * t : SUB * (t + 1)] for t in range(n)]
    out = []
    each = range(SUB)
    for g in range(n):
        c0 = g * SUB
        d = rows[g]
        inside = (lane >= c0) & (lane < c0 + SUB)
        cols = [lane_of(d, c0 + j) for j in each]
        s = {(i, j): row_of(cols[j], i) for j in each for i in range(j, SUB)}
        mixed = jnp.where(inside, jnp.where(lane - c0 == sub, 1.0, 0.0), d)
        u = [row_of(mixed, i) for i in each]
        more = g + 1 < n
        if more:
            below = [lane_of(rows[g + 1], c0 + j) for j in each]
            ahead = jnp.where(inside, 0.0, rows[g + 1])
        m, ur = {}, []
        for k in each:
            r = 1.0 / s[k, k]
            for i in range(k + 1, SUB):
                m[i, k] = s[i, k] * r
            for j in range(k + 1, SUB):
                for i in range(j, SUB):
                    s[i, j] = s[i, j] - m[i, k] * s[j, k]
            ur.append(u[k] * r)
            for i in range(k + 1, SUB):
                u[i] = u[i] - m[i, k] * u[k]
            if more:
                for i in range(k + 1, SUB):
                    below[i] = below[i] - m[i, k] * below[k]
                ahead = ahead - below[k] * ur[k]
        whole, pivot = u[0], s[0, 0]
        for i in range(1, SUB):
            whole = jnp.where(sub == i, u[i], whole)
            pivot = jnp.where(sub == i, s[i, i], pivot)
        out.append(jnp.where(lane < c0 + SUB, whole * lax.rsqrt(pivot), 0.0))
        if not more:
            break
        rows[g + 1] = ahead
        z = [None] * SUB
        for j in reversed(each):
            z[j] = ur[j]
            for i in range(j + 1, SUB):
                z[j] = z[j] - m[i, j] * z[i]
        for t in range(g + 2, n):
            terms = [lane_of(rows[t], c0 + j) * z[j] for j in each]
            rows[t] = jnp.where(inside, 0.0, rows[t]) - tree(terms)
    return jnp.concatenate(out, axis=0)


def factor_kernel(a_ref, b_ref, inv_ref, t_ref):
    t_ref[...] = jnp.zeros_like(t_ref)
    for n, (j, k) in enumerate(UPPER):
        t_ref[j * TILE : (j + 1) * TILE, k * TILE : (k + 1) * TILE] = a_ref[n] + b_ref[n]
    eye = (
        lax.broadcasted_iota(jnp.int32, (TILE, TILE), 0)
        == lax.broadcasted_iota(jnp.int32, (TILE, TILE), 1)
    ).astype(jnp.float32)
    for j in range(TILES):
        t_ref[j * TILE : (j + 1) * TILE, PANEL + j * TILE : PANEL + (j + 1) * TILE] = eye

    @pl.loop(0, TILES)
    def _(j):
        here = pl.ds(pl.multiple_of(j * TILE, TILE), TILE)
        inv = inverse_factor(t_ref[here, here])
        scaled = jnp.dot(
            inv, t_ref[here, :], precision=lax.Precision.HIGHEST, preferred_element_type=jnp.float32
        )
        inv_ref[here, :] = scaled[:, PANEL:]
        lane = lax.broadcasted_iota(jnp.int32, (TILE, PANEL), 1)
        ahead = jnp.where(lane >= (j + 1) * TILE, scaled[:, :PANEL], 0.0).T
        for i in range(1, TILES):

            @pl.when(i > j)
            def _():
                part = slice(i * TILE, (i + 1) * TILE)
                t_ref[part, :] -= jnp.dot(
                    ahead[part],
                    scaled,
                    precision=lax.Precision.HIGHEST,
                    preferred_element_type=jnp.float32,
                )


def inverse_of_factor(mine, other):
    return pl.pallas_call(
        factor_kernel,
        out_shape=jax.ShapeDtypeStruct((PANEL, PANEL), jnp.float32),
        in_specs=[pl.BlockSpec(memory_space=pltpu.VMEM)] * 2,
        out_specs=pl.BlockSpec(memory_space=pltpu.VMEM),
        scratch_shapes=[pltpu.VMEM((PANEL, 2 * PANEL), jnp.float32)],
        cost_estimate=pl.CostEstimate(
            flops=2 * 10**10, bytes_accessed=3 * 10**6, transcendentals=PANEL
        ),
        name="factor",
    )(mine, other)


def general_body(border, barrier, row_counts):
    scen_here, capacity, own_cols = border.shape
    n_scen = lax.axis_size("scen")
    per_owner = PANEL // lax.axis_size("col")
    rows_owned = own_cols // n_scen
    depth = scen_here * capacity
    positions = lax.iota(jnp.int32, capacity)
    weights = jnp.where(positions[None, :] < row_counts[:, None], 1.0 / barrier, jnp.float32(0.0))
    panel_part = jnp.transpose(border[:, :, :per_owner], (2, 0, 1)).reshape(per_owner, depth)
    panel = lax.all_gather(panel_part, "col", axis=0, tiled=True)
    weighted = panel * weights.reshape(1, depth)
    block = jnp.einsum(
        "pr,qr->pq", weighted, panel, precision=lax.Precision.HIGH,
        preferred_element_type=jnp.float32,
    )
    upper = jnp.stack(
        [block[j * TILE : (j + 1) * TILE, k * TILE : (k + 1) * TILE] for j, k in UPPER]
    )
    if n_scen == 2:
        swap = [(0, 1), (1, 0)]
        upper_other = lax.ppermute(upper, "scen", swap)
    else:
        upper_other = lax.psum(upper, "scen") - upper
    part = jnp.einsum(
        "pr,rc->pc", weighted, border.reshape(depth, own_cols), precision=lax.Precision.HIGH,
        preferred_element_type=jnp.float32,
    )
    if n_scen == 2:
        me = lax.axis_index("scen")
        sent = lax.dynamic_slice_in_dim(part, (1 - me) * rows_owned, rows_owned, 1)
        kept = lax.dynamic_slice_in_dim(part, me * rows_owned, rows_owned, 1)
        owned = kept + lax.ppermute(sent, "scen", swap)
    else:
        owned = lax.psum_scatter(part, "scen", scatter_dimension=1, tiled=True)
    inverse = inverse_of_factor(upper, upper_other)
    solved = jnp.einsum(
        "qt,pq->tp", owned, inverse, precision=lax.Precision.HIGHEST,
        preferred_element_type=jnp.float32,
    )
    return solved.reshape(1, 1, rows_owned, PANEL)


MESH = pl.DeviceIdType.MESH
CHUNK = 256
LAG = 3


def split(x):
    hi = x.astype(jnp.bfloat16)
    return hi, (x - hi.astype(jnp.float32)).astype(jnp.bfloat16)


def exact(a, b):
    return jnp.dot(a, b, precision=lax.Precision.HIGHEST, preferred_element_type=jnp.float32)


def bf16_nt(a, b):
    return lax.dot_general(a, b, (((1,), (1,)), ((), ())), preferred_element_type=jnp.float32)


def bf16_nn(a, b):
    return jnp.dot(a, b, preferred_element_type=jnp.float32)


def ring_kernel(
    barrier_ref, counts_ref, border_ref, out_ref,
    pan, part_ref, w_ref, gath, stage, bhi, blo, phi, plo, whi, wlo,
    u_keep, u_send, u_recv, g_own, g_recv, t_ref, inv_ref, low_ref, x_ref,
    pan_sem, stage_sem, ring_send, core_send, recv_sem, uy_send, uy_recv, gy_send, gy_recv, g_push_sem, g_share_send, g_share_recv,
):
    chips = lax.axis_size("col") // 2
    half_ring = chips // 2
    me = lax.axis_index("col")
    scen = lax.axis_index("scen")
    core = me % 2
    chip = me // 2
    pos = (1 - chip % 2) * (chip // 2) + (chip % 2) * (chips - 1 - chip // 2)
    depth_half = part_ref.shape[2]
    per = part_ref.shape[1]
    depth = 2 * depth_half
    cols = border_ref.shape[1]
    rows_owned = cols // 2

    def chip_at(p):
        p = (p + 2 * chips) % chips
        x = p // half_ring
        z = (1 - x) * p + x * (chips - 1 - p)
        return 2 * z + x

    up = {"col": 2 * chip_at(pos + 1) + core}
    down = {"col": 2 * chip_at(pos - 1) + core}
    mate = {"col": 2 * chip + 1 - core}
    across = {"scen": 1 - scen}

    barrier = pltpu.get_barrier_semaphore()
    for peer in (up, down, mate, across):
        pl.semaphore_signal(barrier, inc=1, device_id=peer, device_id_type=MESH)

    def fetch(n):
        return pltpu.make_async_copy(
            border_ref.at[pl.ds(pl.multiple_of(n * CHUNK, CHUNK), CHUNK)],
            stage.at[n % LAG],
            stage_sem.at[n % LAG],
        )

    def fetch_panel(h):
        return pltpu.make_async_copy(
            border_ref.at[pl.ds(h * depth_half, depth_half), pl.ds(0, TILE)],
            pan.at[h],
            pan_sem.at[h],
        )

    chunks = depth // CHUNK
    for h in range(2):
        fetch_panel(h).start()

    def send(src, block, h, send_sem, peer):
        return pltpu.make_async_remote_copy(
            src_ref=src,
            dst_ref=gath.at[block, h],
            send_sem=send_sem,
            recv_sem=recv_sem.at[block, h],
            device_id=peer,
            device_id_type=MESH,
        )

    def own(h, d):
        sem = core_send.at[0, h] if d == 2 else ring_send.at[d, 0, h]
        return send(part_ref.at[h], me, h, sem, (up, down, mate)[d])

    def block_of(d, k):
        return 2 * chip_at(pos - k if d == 0 else pos + k) + core

    def forward(d, k, h):
        block = block_of(d, k)
        return send(gath.at[block, h], block, h, ring_send.at[d, k, h], (up, down)[d])

    def push(d, k, h):
        block = block_of(d, k)
        return send(gath.at[block, h], block, h, core_send.at[2 * k - d, h], mate)

    def arrived(block, h):
        pltpu.make_async_copy(part_ref.at[h], gath.at[block, h], recv_sem.at[block, h]).wait()

    for h in range(2):
        fetch_panel(h).wait()
        for n in range(depth_half // TILE):
            here = slice(n * TILE, (n + 1) * TILE)
            part_ref[h, :, here] = pan[h, here, :].T[:per]
        if h == 0:
            pl.semaphore_wait(barrier, 4)
        for d in range(3):
            own(h, d).start()
    for n in range(LAG):
        fetch(n).start()
    place = lax.broadcasted_iota(jnp.int32, (1, depth_half), 1)
    for h in range(2):
        w_ref[h : h + 1, :] = jnp.where(place < counts_ref[h], 1.0 / barrier_ref[h : h + 1, :], 0.0)

    def convert_border(first):
        @pl.loop(first, first + chunks // 2)
        def _(n):
            fetch(n).wait()
            here = pl.ds(pl.multiple_of(n * CHUNK, CHUNK), CHUNK)
            hi, lo = split(stage[n % LAG])
            bhi[here, :] = hi
            blo[here, :] = lo

            @pl.when(n + LAG < chunks)
            def _():
                fetch(n + LAG).start()

    def convert(which, cc, src):
        for h in range(2):
            there = (which, pl.ds(cc * per, per), pl.ds(h * depth_half, depth_half))
            x = src(h)
            phi[there], plo[there] = split(x)
            whi[there], wlo[there] = split(x * w_ref[h : h + 1, :])

    def convert_both(which):
        for cc in range(2):
            convert(which, cc, lambda h: gath[2 * which + cc, h])

    def product(unit, which, dst, unroll=False):
        left = jnp.concatenate([ref[a] for ref in (whi, wlo) for a in unit], axis=0)
        rows = left.shape[0] // 2
        each = whi.shape[1]

        def columns(n):
            col = pl.ds(pl.multiple_of(which * rows_owned + n * CHUNK, CHUNK), CHUNK)
            to = pl.ds(pl.multiple_of(n * CHUNK, CHUNK), CHUNK)
            both = bf16_nn(left, bhi[:, col])
            res = both[:rows] + both[rows:] + bf16_nn(left[:rows], blo[:, col])
            for i, a in enumerate(unit):
                dst[a, :, to] = res[i * each : (i + 1) * each]

        if unroll:
            for n in range(rows_owned // CHUNK):
                columns(n)
        else:
            pl.loop(0, rows_owned // CHUNK)(columns)

    def cross(which):
        return pltpu.make_async_remote_copy(
            src_ref=u_send.at[which],
            dst_ref=u_recv.at[which],
            send_sem=uy_send.at[which],
            recv_sem=uy_recv.at[which],
            device_id=across,
            device_id_type=MESH,
        )

    def product_send(unit, unroll=False):
        product(unit, 1 - scen, u_send, unroll)
        for which in unit:
            cross(which).start()

    def g_at(n):
        row = max(n - 1, 0)
        first, last = (0, TILE) if n == 0 else (max(row, 1) * TILE, PANEL)
        return row, slice(None), slice(first, last)

    def g_owner(n):
        return (n // 2) % 2

    def g_share(n):
        return pltpu.make_async_remote_copy(
            src_ref=g_own.at[g_at(n)],
            dst_ref=g_own.at[g_at(n)],
            send_sem=g_share_send.at[n],
            recv_sem=g_share_recv.at[n],
            device_id=mate,
            device_id_type=MESH,
        )

    def g_push(n):
        return pltpu.make_async_remote_copy(
            src_ref=g_recv.at[g_at(n)],
            dst_ref=g_recv.at[g_at(n)],
            send_sem=g_push_sem.at[n],
            recv_sem=gy_recv.at[n],
            device_id=mate,
            device_id_type=MESH,
        )

    def g_relay(n):
        @pl.when(core == g_owner(n))
        def _():
            g_piece(n).wait_recv()
            g_push(n).start()

    def g_wait(n):
        @pl.when(core != g_owner(n))
        def _():
            g_piece(n).wait_recv()
            g_share(n).wait_recv()

    def g_piece(n):
        at = g_at(n)
        return pltpu.make_async_remote_copy(
            src_ref=g_own.at[at],
            dst_ref=g_recv.at[at],
            send_sem=gy_send.at[n],
            recv_sem=gy_recv.at[n],
            device_id=across,
            device_id_type=MESH,
        )

    def gram(n):
        row, _, lanes = g_at(n)
        left = jnp.concatenate(
            [ref[2 * row + a] for ref in (whi, wlo) for a in range(2)], axis=0
        )
        pairs = slice(2 * lanes.start // TILE, 2 * lanes.stop // TILE)
        right_hi = phi[pairs].reshape(lanes.stop - lanes.start, depth)
        right_lo = plo[pairs].reshape(lanes.stop - lanes.start, depth)
        both = bf16_nt(left, right_hi)
        g_own[g_at(n)] = both[:TILE] + both[TILE:] + bf16_nt(left[:TILE], right_lo)
        g_piece(n).start()
        if n > 0:
            g_share(n).start()

    def receive(d, k, h, first):
        block = block_of(d, k)
        arrived(block, h)
        push(d, k, h).start()

        @pl.when(k < half_ring - 1 + first)
        def _():
            forward(d, k, h).start()

    @pl.loop(1, half_ring)
    def _(k):
        @pl.when(k == 1)
        def _():
            convert_border(0)

        receive(0, k, 0, 1)
        receive(1, k, 0, 0)

        @pl.when(k == 1)
        def _():
            convert_border(chunks // 2)
            for h in range(2):
                arrived(2 * chip + 1 - core, h)
            convert(chip, core, lambda h: part_ref[h])
            convert(chip, 1 - core, lambda h: gath[2 * chip + 1 - core, h])
            product_send([chip])

        before = [chip_at(pos - k + 1), chip_at(pos + k - 1)]

        @pl.when(k > 1)
        def _():
            product_send(before)

        receive(1, k, 1, 1)
        receive(0, k, 1, 0)

        @pl.when(k == 1)
        def _():
            product([chip], scen, u_keep)

        @pl.when(k > 1)
        def _():
            product(before, scen, u_keep)

        for d in range(2):
            which = block_of(d, k) // 2
            for h in range(2):
                arrived(2 * which + 1 - core, h)
            convert_both(which)

    last = [chip_at(pos - half_ring + 1), chip_at(pos + half_ring - 1)]
    far = chip_at(pos + half_ring)
    product_send(last)
    for h in range(2):
        arrived(block_of(h, half_ring), h)
        push(h, half_ring, h).start()
    product(last, scen, u_keep)
    for h in range(2):
        arrived(2 * far + 1 - core, h)
    convert_both(far)
    gram(0)
    for owner in range(2):

        @pl.when(core == owner)
        def _():
            for n in range(1, TILES + 1):
                if g_owner(n) == owner:
                    gram(n)

    t_ref[...] = jnp.zeros_like(t_ref)

    def tiles(i):
        return slice(i * TILE, (i + 1) * TILE)

    g_piece(0).wait_recv()
    inv = inverse_factor(g_own[0, :, :TILE] + g_recv[0, :, :TILE])
    product([far], 1 - scen, u_send, True)
    cross(far).start()
    g_relay(1)
    g_relay(2)
    product([far], scen, u_keep, True)
    g_relay(3)
    g_relay(4)
    g_wait(1)
    t_ref[:TILE, TILE:] += g_own[0, :, TILE:] + g_recv[0, :, TILE:]
    for j in range(TILES):
        inv_ref[j] = inv
        if j == TILES - 1:
            break
        scaled = exact(inv, t_ref[tiles(j), (j + 1) * TILE :])
        ahead = scaled.T
        low_ref[(j + 1) * TILE :, tiles(j)] = ahead
        g_wait(j + 2)
        right = slice((j + 1) * TILE, PANEL)
        t_ref[tiles(j + 1), right] += g_own[j + 1, :, right] + g_recv[j + 1, :, right]
        if j == TILES - 2:
            for which in range(chips):
                cross(which).wait_recv()
        pivot = t_ref[tiles(j + 1), tiles(j + 1)] - exact(ahead[:TILE], scaled[:, :TILE])
        inv = inverse_factor(pivot)
        for i in range(j + 1, TILES):
            first = max(i, j + 2)
            if first < TILES:
                t_ref[tiles(i), first * TILE :] -= exact(
                    ahead[tiles(i - j - 1)], scaled[:, (first - j - 1) * TILE :]
                )
        if j == TILES - 2:
            for i in range(TILES):
                pair = slice(2 * i, 2 * i + 2)
                x_ref[tiles(i), :] = (u_keep[pair] + u_recv[pair]).reshape(TILE, rows_owned)
            for i in range(TILES - 1):
                x = exact(inv_ref[i], x_ref[tiles(i), :])
                out_ref[:, tiles(i)] = x.T
                x_ref[(i + 1) * TILE :, :] -= exact(low_ref[(i + 1) * TILE :, tiles(i)], x)
    out_ref[:, tiles(TILES - 1)] = exact(inv, x_ref[tiles(TILES - 1), :]).T

    for h in range(2):
        for d in range(3):
            own(h, d).wait_send()
    for k in range(1, half_ring + 1):
        for d in range(2):
            for h in range(2):
                if k < half_ring - 1 or (k < half_ring and d == h):
                    forward(d, k, h).wait_send()
                if k < half_ring or d == h:
                    push(d, k, h).wait_send()
    for which in range(chips):
        cross(which).wait_send()
    g_piece(0).wait_send()
    for n in range(1, TILES + 1):

        @pl.when(core == g_owner(n))
        def _():
            g_piece(n).wait_send()
            g_push(n).wait_send()
            g_share(n).wait_send()


def ring_body(border, barrier, row_counts):
    scen_here, capacity, own_cols = border.shape
    n_col = lax.axis_size("col")
    chips = n_col // 2
    per = PANEL // n_col
    depth = scen_here * capacity
    rows_owned = own_cols // lax.axis_size("scen")
    dma = pltpu.SemaphoreType.DMA
    f32, bf16 = jnp.float32, jnp.bfloat16
    solved = pl.pallas_call(
        ring_kernel,
        out_shape=jax.ShapeDtypeStruct((rows_owned, PANEL), f32),
        in_specs=[
            pl.BlockSpec(memory_space=pltpu.VMEM),
            pl.BlockSpec(memory_space=pltpu.SMEM),
            pl.BlockSpec(memory_space=pl.ANY),
        ],
        out_specs=pl.BlockSpec(memory_space=pltpu.VMEM),
        scratch_shapes=[
            pltpu.VMEM((scen_here, capacity, TILE), f32),
            pltpu.VMEM((scen_here, per, capacity), f32),
            pltpu.VMEM((scen_here, capacity), f32),
            pltpu.VMEM((n_col, scen_here, per, capacity), f32),
            pltpu.VMEM((LAG, CHUNK, own_cols), f32),
            pltpu.VMEM((depth, own_cols), bf16),
            pltpu.VMEM((depth, own_cols), bf16),
            *[pltpu.VMEM((chips, 2 * per, depth), bf16)] * 4,
            *[pltpu.VMEM((chips, 2 * per, rows_owned), f32)] * 3,
            *[pltpu.VMEM((TILES, TILE, PANEL), f32)] * 2,
            pltpu.VMEM((PANEL, PANEL), f32),
            pltpu.VMEM((TILES, TILE, TILE), f32),
            pltpu.VMEM((PANEL, PANEL), f32),
            pltpu.VMEM((PANEL, rows_owned), f32),
            dma((scen_here,)),
            dma((LAG,)),
            dma((2, chips // 2, 2)),
            dma((chips + 1, 2)),
            dma((n_col, 2)),
            dma((chips,)),
            dma((chips,)),
            *[dma((TILES + 1,))] * 5,
        ],
        compiler_params=pltpu.CompilerParams(
            collective_id=0, has_side_effects=True, vmem_limit_bytes=50 * 2**20
        ),
        name="ring",
    )(barrier, row_counts, border.reshape(depth, own_cols))
    return solved.reshape(1, 1, rows_owned, PANEL)


def solution(mesh):
    n_scen, n_col = mesh.shape["scen"], mesh.shape["col"]
    ring = n_scen == 2 and 4 * (PANEL // n_col) == TILE
    placed = (P("scen", None, "col"), P("scen", None), P("scen"))
    return jax.shard_map(
        ring_body if ring else general_body,
        mesh=mesh,
        in_specs=placed,
        out_specs=P("col", "scen", None, None),
        check_vma=False,
    )
```
